1024 devices in a mesh: row: 8 (over y, core), col: 16 (over z_lo), layer: 8 (over z_hi, x).
Axes of the slice: x: 4, y: 4, z: 32 (z_hi: 2, z_lo: 16; z = z_hi * 16 + z_lo), core: 2. Of those that a mesh axis runs over, the one named last changes fastest.
Arguments:
- a_values: bfloat16 [8, 8, 16, 2, 256, 256], P('row', 'layer', 'col'), may hold values from -0.375 to 0.375
- a_index: int32 [8, 8, 16, 2, 2], P('row', 'layer', 'col'), may hold values from 0 to 15, as said below
- a_count: int32 [8, 8, 16], P('row', 'layer', 'col'), may hold values from 0 to 2, as said below
- b_values: bfloat16 [8, 8, 16, 256, 2, 256], P('layer', 'row', 'col'), may hold values from -6 to 6
- b_index: int32 [8, 8, 16, 2, 2], P('layer', 'row', 'col'), may hold values from 0 to 7, as said below
- b_count: int32 [8, 8, 16], P('layer', 'row', 'col'), may hold values from 0 to 2, as said below
- c_index: int32 [8, 16, 2, 16], P('row', 'col'), may hold values from 0 to 15, as said below
- c_count: int32 [8, 16], P('row', 'col'), may hold values from 0 to 16, as said below
Outputs:
- c_blocks: float32 [8, 16, 16, 256, 256], P('row', 'col', 'layer')
The draws below stay inside these ranges and needn't reach their ends.
Inputs may be any that keep to these rules, and one draw needn't show every extreme that they name: a_count is at most 2 and equals it for some tile; the first a_count slots of a tile name distinct blocks; each block row of A has exactly 1 stored blocks in every inner range. `a_index`: row entries lie below 16, inner entries below 1. b_count is at most 2 and equals it for some tile; the first b_count slots of a tile name distinct blocks; each block column of B has either no stored block or exactly 1 stored blocks in every inner range. `b_index`: inner entries lie below 2, column entries below 8. c_count is at most 16 and equals it for some tile; the first c_count slots of a tile name distinct blocks; the target pattern is exactly the set of blocks that the product A B reaches, and each of them receives exactly 1 block products in every inner range. `c_index`: row entries lie below 16, column entries below 8.
All inputs are finite; a program needn't handle non-finite values.
Results may differ from the reference program's by a relative error of at most 0.01.
Values may be sent and summed in bfloat16 or wider, within the bound.
A program may use at most 64 MiB of HBM per device.

```python
import jax
import jax.numpy as jnp
from jax import lax

BLOCK = 256
NB = 128
ROW_TILES = 8
COL_TILES = 16
LAYERS = 8
ROW_BLOCKS = 16
COL_BLOCKS = 8
KA_BLOCKS = 1
KB_BLOCKS = 2
A_SLOTS = 2
B_SLOTS = 2
C_SLOTS = 16


def class_tables(key):
    base = jax.random.fold_in(key, 4242)
    classes = ROW_BLOCKS
    inner = NB // LAYERS
    half = ROW_BLOCKS // 2
    leading = jax.random.permutation(jax.random.fold_in(base, 1), classes).astype(jnp.int32)
    row_star = jax.random.randint(jax.random.fold_in(base, 2), (), 0, ROW_TILES)
    col_star = jax.random.randint(jax.random.fold_in(base, 3), (), 0, COL_TILES)
    layer_star = jax.random.randint(jax.random.fold_in(base, 4), (), 0, LAYERS)
    band_star = jax.random.randint(jax.random.fold_in(base, 5), (), 0, ROW_TILES)
    doubled = jnp.concatenate([jnp.arange(classes, dtype=jnp.int32), jnp.arange(classes, dtype=jnp.int32)])
    row_keys = jax.random.split(jax.random.fold_in(base, 6), ROW_TILES)
    drawn_rows = jax.vmap(lambda single: jax.random.permutation(single, doubled)[:ROW_BLOCKS])(row_keys)
    forced_rows = jax.random.permutation(jax.random.fold_in(base, 7), jnp.concatenate([leading[:half], leading[:half]]))
    row_pick = (jnp.arange(ROW_TILES, dtype=jnp.int32) == row_star)[:, None]
    row_classes = jnp.where(row_pick, forced_rows[None, :], drawn_rows).astype(jnp.int32)
    col_keys = jax.random.split(jax.random.fold_in(base, 8), COL_TILES)
    drawn_cols = jax.vmap(lambda single: jax.random.permutation(single, classes)[:COL_BLOCKS])(col_keys)
    empty_cols = jax.random.randint(jax.random.fold_in(base, 11), (COL_TILES, COL_BLOCKS), 0, 4) == 0
    drawn_cols = jnp.where(empty_cols, -1, drawn_cols).astype(jnp.int32)
    forced_cols = jax.random.permutation(jax.random.fold_in(base, 9), leading[:COL_BLOCKS])
    col_pick = (jnp.arange(COL_TILES, dtype=jnp.int32) == col_star)[:, None]
    col_classes = jnp.where(col_pick, forced_cols[None, :], drawn_cols).astype(jnp.int32)
    layer_keys = jax.random.split(jax.random.fold_in(base, 10), LAYERS)
    drawn_inner = jax.vmap(lambda single: jax.random.permutation(single, inner) % classes)(layer_keys)
    shifted = (jnp.arange(inner, dtype=jnp.int32) - band_star * KB_BLOCKS) % inner % classes
    forced_inner = leading[shifted]
    layer_pick = (jnp.arange(LAYERS, dtype=jnp.int32) == layer_star)[:, None]
    inner_classes = jnp.where(layer_pick, forced_inner[None, :], drawn_inner).astype(jnp.int32)
    return (row_classes, col_classes, inner_classes)


def slot_lists(key, present, slots):
    tiles, positions = present.shape
    keys = jax.random.split(key, tiles)
    ranks = jax.vmap(lambda single: jax.random.permutation(single, positions))(keys).astype(jnp.int32)
    scores = jnp.where(present, 0, positions).astype(jnp.int32) + ranks
    order = jnp.argsort(scores, axis=1, stable=True).astype(jnp.int32)
    counts = jnp.sum(present.astype(jnp.int32), axis=1).astype(jnp.int32)
    return (order[:, :slots], counts)


def left_lists(key):
    row_classes, col_classes, inner_classes = class_tables(key)
    inner_tiles = inner_classes.reshape(LAYERS, COL_TILES, KA_BLOCKS)
    present = row_classes[:, None, None, :, None] == inner_tiles[None, :, :, None, :]
    present = present.reshape(ROW_TILES * LAYERS * COL_TILES, ROW_BLOCKS * KA_BLOCKS)
    return slot_lists(jax.random.fold_in(key, 101), present, A_SLOTS)


def right_lists(key):
    row_classes, col_classes, inner_classes = class_tables(key)
    inner_tiles = inner_classes.reshape(LAYERS, ROW_TILES, KB_BLOCKS)
    present = inner_tiles[:, :, None, :, None] == col_classes[None, None, :, None, :]
    present = present.reshape(LAYERS * ROW_TILES * COL_TILES, KB_BLOCKS * COL_BLOCKS)
    return slot_lists(jax.random.fold_in(key, 202), present, B_SLOTS)


def target_lists(key):
    row_classes, col_classes, inner_classes = class_tables(key)
    present = row_classes[:, None, :, None] == col_classes[None, :, None, :]
    present = present.reshape(ROW_TILES * COL_TILES, ROW_BLOCKS * COL_BLOCKS)
    return slot_lists(jax.random.fold_in(key, 303), present, C_SLOTS)


def draw_a_index(key, part):
    chosen, _ = left_lists(key)
    stacked = jnp.stack([chosen // KA_BLOCKS, chosen % KA_BLOCKS], axis=1)
    return stacked.reshape(ROW_TILES, LAYERS, COL_TILES, 2, A_SLOTS).astype(jnp.int32)


def draw_a_count(key, part):
    _, counts = left_lists(key)
    return counts.reshape(ROW_TILES, LAYERS, COL_TILES).astype(jnp.int32)


def draw_b_index(key, part):
    chosen, _ = right_lists(key)
    stacked = jnp.stack([chosen // COL_BLOCKS, chosen % COL_BLOCKS], axis=1)
    return stacked.reshape(LAYERS, ROW_TILES, COL_TILES, 2, B_SLOTS).astype(jnp.int32)


def draw_b_count(key, part):
    _, counts = right_lists(key)
    return counts.reshape(LAYERS, ROW_TILES, COL_TILES).astype(jnp.int32)


def draw_c_index(key, part):
    chosen, _ = target_lists(key)
    stacked = jnp.stack([chosen // COL_BLOCKS, chosen % COL_BLOCKS], axis=1)
    return stacked.reshape(ROW_TILES, COL_TILES, 2, C_SLOTS).astype(jnp.int32)


def draw_c_count(key, part):
    _, counts = target_lists(key)
    return counts.reshape(ROW_TILES, COL_TILES).astype(jnp.int32)


def levels(stream_key, shape, cuts, smallest, top_value):
    def one(dim, parts):
        steps = jax.random.uniform(jax.random.fold_in(jax.random.fold_in(stream_key, 6), dim), (parts,), jnp.float32, smallest / len(cuts), top_value / len(cuts))
        return jnp.repeat(jnp.exp(steps), shape[dim] // parts).reshape((-1,) + (1,) * (len(shape) - dim - 1))

    gain = one(*cuts[0])
    for cut in cuts[1:]:
        gain = gain * one(*cut)
    return gain


def bell_draw(key, extent, width, limit, cuts=(), kind=jnp.bfloat16):
    entries = width * jax.random.normal(key, extent, jnp.float32)
    if cuts:
        entries = entries * levels(key, extent, cuts, -0.22, 0.18)
    return jnp.clip(entries, -limit, limit).astype(kind)


def setup_inputs(seed: int = 0) -> dict:
    splits = jax.random.split(jax.random.key(seed), 9)
    a_values = bell_draw(splits[0], (ROW_TILES, LAYERS, COL_TILES, A_SLOTS, BLOCK, BLOCK), BLOCK ** -0.5, 0.375, ((0, 8), (1, 8), (2, 16)))
    a_index = draw_a_index(jax.random.fold_in(splits[8], 71), 0)
    a_count = draw_a_count(jax.random.fold_in(splits[8], 71), 0)
    b_values = bell_draw(splits[3], (LAYERS, ROW_TILES, COL_TILES, BLOCK, B_SLOTS, BLOCK), 1.0, 6.0, ((0, 8), (1, 8), (2, 16)))
    b_index = draw_b_index(jax.random.fold_in(splits[8], 71), 0)
    b_count = draw_b_count(jax.random.fold_in(splits[8], 71), 0)
    c_index = draw_c_index(jax.random.fold_in(splits[8], 71), 0)
    c_count = draw_c_count(jax.random.fold_in(splits[8], 71), 0)
    return dict(a_values=a_values, a_index=a_index, a_count=a_count, b_values=b_values, b_index=b_index, b_count=b_count, c_index=c_index, c_count=c_count)


def pair_terms(totals, left_blocks, left_index, left_count, left_tile, right_blocks, right_index, right_count, right_tile, target):
    pattern_rows, pattern_cols, pattern_live, ka_blocks, kb_blocks = target
    left_slots = left_blocks.shape[0]
    right_slots = right_blocks.shape[1]
    slot_count = totals.shape[0]
    left_live = jnp.arange(left_slots, dtype=jnp.int32) < left_count
    right_live = jnp.arange(right_slots, dtype=jnp.int32) < right_count
    left_depth = left_tile * ka_blocks + left_index[1]
    right_depth = right_tile * kb_blocks + right_index[0]
    matched = left_live[:, None, None] & right_live[None, :, None]
    matched = matched & (left_depth[:, None, None] == right_depth[None, :, None])
    matched = matched & (left_index[0][:, None, None] == pattern_rows[None, None, :])
    matched = matched & (right_index[1][None, :, None] == pattern_cols[None, None, :])
    matched = matched & pattern_live[None, None, :]
    pair_hits = matched.reshape(left_slots * right_slots, slot_count)
    pair_live = jnp.any(pair_hits, axis=1)
    slot_of = jnp.sum(pair_hits.astype(jnp.int32) * jnp.arange(slot_count, dtype=jnp.int32)[None, :], axis=1).astype(jnp.int32)
    pair_order = jnp.argsort(jnp.where(pair_live, 0, 1).astype(jnp.int32), stable=True).astype(jnp.int32)
    live_pairs = jnp.sum(pair_live.astype(jnp.int32)).astype(jnp.int32)

    def add_pair(position, running):
        pair_id = pair_order[position]
        left_one = lax.dynamic_index_in_dim(left_blocks, pair_id // right_slots, 0, False)
        right_one = lax.dynamic_index_in_dim(right_blocks, pair_id % right_slots, 1, False)
        product = jnp.dot(left_one, right_one, preferred_element_type=jnp.float32)
        target_slot = slot_of[pair_id]
        previous = lax.dynamic_index_in_dim(running, target_slot, 0, False)
        return lax.dynamic_update_index_in_dim(running, previous + product, target_slot, 0)

    return lax.fori_loop(jnp.int32(0), live_pairs, add_pair, totals)


def reference(a_values, a_index, a_count, b_values, b_index, b_count, c_index, c_count):
    ratio_tiles = KB_BLOCKS // KA_BLOCKS

    def one_tile(tile_id):
        tile_row = tile_id // COL_TILES
        tile_col = tile_id % COL_TILES
        pattern_live = jnp.arange(C_SLOTS, dtype=jnp.int32) < c_count[tile_row, tile_col]
        target = (c_index[tile_row, tile_col, 0], c_index[tile_row, tile_col, 1], pattern_live, KA_BLOCKS, KB_BLOCKS)
        zeros_start = jnp.zeros((C_SLOTS, BLOCK, BLOCK), jnp.float32)

        def one_layer(summed, layer_id):
            def one_source(source, running):
                right_tile = source // ratio_tiles
                return pair_terms(running, a_values[tile_row, layer_id, source], a_index[tile_row, layer_id, source], a_count[tile_row, layer_id, source], source, b_values[layer_id, right_tile, tile_col], b_index[layer_id, right_tile, tile_col], b_count[layer_id, right_tile, tile_col], right_tile, target)

            partial_value = lax.fori_loop(0, COL_TILES, one_source, zeros_start)
            rounded = lax.optimization_barrier(partial_value.astype(jnp.bfloat16))
            return summed + rounded.astype(jnp.float32), None

        summed, _ = lax.scan(one_layer, zeros_start, jnp.arange(LAYERS, dtype=jnp.int32))
        return summed

    blocks = lax.map(one_tile, jnp.arange(ROW_TILES * COL_TILES, dtype=jnp.int32))
    return blocks.reshape(ROW_TILES, COL_TILES, C_SLOTS, BLOCK, BLOCK)
```

```python
import functools

import jax
import jax.numpy as jnp
from jax import lax
from jax.experimental import pallas as pl
from jax.experimental.pallas import tpu as pltpu
from jax.sharding import Mesh
from jax.sharding import PartitionSpec as P

LAYER = ("layer_0", "layer_1")
MESH = pl.DeviceIdType.MESH
B_ROWS, B_CORES = 6, 8


def kernel(
    sizes,
    a_idx,
    a_cnt,
    b_idx,
    b_cnt,
    c_idx,
    c_cnt,
    a_in,
    b_in,
    out,
    a_all,
    a_meta,
    a_tab,
    b_all,
    b_meta,
    b_tab,
    b_hop,
    b_far,
    parts_out,
    parts_in,
    local_sem,
    a_send,
    a_recv,
    m_send,
    m_recv,
    y_send,
    y_recv,
    d_send,
    d_recv,
    h_send,
    h_recv,
    x_send,
    x_recv,
):
    row_count, col_count, x_count = sizes
    y_count = row_count // 2
    z_count = 2 * col_count
    reach = z_count // 2
    half = a_in.shape[1] // 2
    row, col = lax.axis_index("row"), lax.axis_index("col")
    high, x = lax.axis_index("layer_0"), lax.axis_index("layer_1")
    y, core = row // 2, row % 2
    z = high * col_count + col

    def at_z(step):
        there = (z + step + z_count) % z_count
        return {"layer_0": there // col_count, "col": there % col_count}

    def row_at(step, which):
        return ((y + step + y_count) % y_count) * 2 + which

    def at_row(step, which):
        return {"row": row_at(step, which)}

    def at_x(step):
        return {"layer_1": (x + step) % x_count}

    def send(src, dst, send_sem, recv_sem, where):
        copy = pltpu.make_async_remote_copy(
            src_ref=src, dst_ref=dst, send_sem=send_sem, recv_sem=recv_sem, device_id=where, device_id_type=MESH
        )
        copy.start()
        sent.append(copy)

    def arrived(ref, sem):
        pltpu.make_async_copy(ref, ref, sem).wait()

    sent = []

    own_a = pltpu.make_async_copy(a_in, a_all.at[pl.ds(0, 2)], local_sem.at[0])
    own_b = pltpu.make_async_copy(b_in, b_all.at[pl.ds(2 * row, 2)], local_sem.at[1])
    own_a.start()
    own_b.start()
    lane = lax.broadcasted_iota(jnp.int32, (1, 128), 1)
    listed = jnp.zeros((1, 128), jnp.int32)
    for place, value in enumerate((a_idx[0], a_idx[1], a_cnt[0], b_idx[2], b_idx[3], b_cnt[0])):
        listed = jnp.where(lane == place, value, listed)
    a_meta[0] = listed
    b_meta[row] = listed

    barrier = pltpu.get_barrier_semaphore()
    partners = [at_z(1), at_z(-1), at_row(0, 1 - core)]
    partners += [at_row(step, core) for step in range(1, y_count)]
    partners += [at_x(step) for step in range(1, x_count)]
    for partner in partners:
        pl.semaphore_signal(barrier, inc=1, device_id=partner, device_id_type=MESH)
    own_a.wait()
    own_b.wait()
    pl.semaphore_wait(barrier, len(partners))

    def rows_from(step, which):
        return b_all.at[pl.ds(2 * row_at(-step, which), 2)], b_meta.at[row_at(-step, which)]

    def b_over_y():
        tile, lists = rows_from(0, core)
        for step in range(1, y_count):
            send(lists, lists, y_send.at[0, step], y_recv.at[0, step], at_row(step, core))
            send(tile, tile, y_send.at[1, step], y_recv.at[1, step], at_row(step, core))
        send(lists, lists, d_send.at[0, 0], d_recv.at[0, 0], at_row(0, 1 - core))
        send(tile, tile, d_send.at[1, 0], d_recv.at[1, 0], at_row(0, 1 - core))

    def b_over_cores():
        for step in range(1, y_count):
            tile, lists = rows_from(step, core)
            arrived(lists, y_recv.at[0, step])
            arrived(tile, y_recv.at[1, step])
            send(lists, lists, d_send.at[0, step], d_recv.at[0, step], at_row(0, 1 - core))
            send(tile, tile, d_send.at[1, step], d_recv.at[1, step], at_row(0, 1 - core))

    def b_gathered():
        for step in range(y_count):
            tile, lists = rows_from(step, 1 - core)
            arrived(lists, d_recv.at[0, step])
            arrived(tile, d_recv.at[1, step])
        table = pltpu.make_async_copy(b_meta, b_tab, local_sem.at[2])
        table.start()
        table.wait()

    def place_of_b(column):
        place = jnp.int32(0)
        for r in range(row_count):
            for slot in range(2):
                hit = (b_tab[r, 0, 3 + slot] == column) & (slot < b_tab[r, 0, 5])
                place = jnp.where(hit, 2 * r + slot, place)
        return place

    def b_hop_send(hop, side):
        src = b_hop.at[side, hop]
        if hop + 1 < reach:
            dst = b_hop.at[side, hop + 1]
        else:
            dst = b_far.at[row, pl.ds(side * half, half)]
        send(src, dst, h_send.at[side, hop], h_recv.at[side, hop], at_z(1 - 2 * side))

    def b_turn():
        b_gathered()
        block = b_all[place_of_b(row)]
        b_hop[0, 0] = block[:half]
        b_hop[1, 0] = block[half:]
        for side in range(2):
            b_hop_send(0, side)

    def b_forward(hop):
        for side in range(2):
            arrived(b_hop.at[side, hop], h_recv.at[side, hop - 1])
            b_hop_send(hop, side)

    def b_far_over_y():
        for side in range(2):
            arrived(b_far.at[row, pl.ds(side * half, half)], h_recv.at[side, reach - 1])
        block = b_far.at[row]
        for step in range(1, y_count):
            send(block, block, y_send.at[2, step], y_recv.at[2, step], at_row(step, core))
        send(block, block, d_send.at[2, 0], d_recv.at[2, 0], at_row(0, 1 - core))

    def b_far_over_cores():
        for step in range(1, y_count):
            block = b_far.at[row_at(-step, core)]
            arrived(block, y_recv.at[2, step])
            send(block, block, d_send.at[2, step], d_recv.at[2, step], at_row(0, 1 - core))

    def b_far_gathered():
        for step in range(y_count):
            arrived(b_far.at[row_at(-step, 1 - core)], d_recv.at[2, step])

    def a_slot(side, tick):
        step, slot = tick // 2, tick % 2
        if step == reach - 1:
            slot = side
        offset = (z_count - step) % z_count if side == 0 else step
        beyond = z_count - step - 1 if side == 0 else step + 1
        return 2 * offset + slot, 2 * beyond + slot

    def a_tick(tick):
        for side in range(2):
            here, there = a_slot(side, tick)
            if tick >= 2:
                before = tick - 2
                if tick // 2 == reach - 1:
                    before = tick - 2 + side
                arrived(a_all.at[here], a_recv.at[side, before])
                waited.add((side, before))
            send(a_all.at[here], a_all.at[there], a_send.at[side, tick], a_recv.at[side, tick], at_z(1 - 2 * side))

    def lists_step(step):
        for side in range(2):
            offset = (z_count - step) % z_count if side == 0 else step
            beyond = z_count - step - 1 if side == 0 else step + 1
            if step == reach - 1 and side == 1:
                continue
            if step >= 1:
                arrived(a_meta.at[offset], m_recv.at[side, step - 1])
            send(a_meta.at[offset], a_meta.at[beyond], m_send.at[side, step], m_recv.at[side, step], at_z(1 - 2 * side))

    def lists_done():
        last = reach - 1
        arrived(a_meta.at[z_count - last - 1], m_recv.at[0, last])
        if last >= 1:
            arrived(a_meta.at[last], m_recv.at[1, last - 1])
        table = pltpu.make_async_copy(a_meta, a_tab, local_sem.at[3])
        table.start()
        table.wait()

    orders = [step for step in (2, 1, 3) if step < x_count] + [0]
    wanted = []

    def find_blocks():
        slots = []
        for step in orders:
            for slot in range(2):
                s = high * 2 * x_count + 2 * ((x + step) % x_count) + slot
                slots.append((step, slot, c_idx[0, s], c_idx[1, s]))

        def look(o, places):
            in_high = ((z + o) % z_count) // col_count
            other = in_high != high
            places = list(places)
            for which in range(2):
                found = a_tab[o, 0, which]
                live = which < a_tab[o, 0, 2]
                here = 2 * o + which
                for n, (_, _, i, _) in enumerate(slots):
                    hit = live & (found == i)
                    places[2 * n] = jnp.where(hit & jnp.logical_not(other), here, places[2 * n])
                    places[2 * n + 1] = jnp.where(hit & other, here, places[2 * n + 1])
            return tuple(places)

        places = lax.fori_loop(0, z_count, look, (jnp.int32(0),) * (2 * len(slots)))
        for n, (step, slot, _, j) in enumerate(slots):
            wanted.append((step, slot, places[2 * n], places[2 * n + 1], place_of_b(j), j))

    waited = set()
    ticks = 2 * reach - 1
    turn = B_CORES
    stages = [(-1, b_over_y), (B_ROWS, b_over_cores), (B_CORES, b_turn)]
    stages += [(B_CORES + hop, functools.partial(b_forward, hop)) for hop in range(1, reach)]
    stages += [(B_CORES + reach, b_far_over_y)]
    stages += [(B_CORES + reach + 3, b_far_over_cores), (B_CORES + reach + 5, b_far_gathered)]
    stages += [(step, functools.partial(lists_step, step)) for step in range(reach)]
    stages += [(turn + reach, lists_done), (turn + reach + 1, find_blocks)]
    stages.sort(key=lambda pair: pair[0])
    for tick in range(ticks):
        while stages and stages[0][0] < tick:
            stages.pop(0)[1]()
        a_tick(tick)
    for _, stage in stages:
        stage()
    for side in range(2):
        for tick in range(ticks):
            if (side, tick) not in waited:
                arrived(a_all.at[a_slot(side, tick)[1]], a_recv.at[side, tick])

    for step, slot, near, far, b_near, j in wanted:
        total = jnp.dot(a_all[near], b_all[b_near], preferred_element_type=jnp.float32)
        total += jnp.dot(a_all[far], b_far[j], preferred_element_type=jnp.float32)
        if step == 0:
            out[slot] = total
        else:
            parts_out[step, slot] = total.astype(jnp.bfloat16)
        if step != 0 and slot == 1:
            send(parts_out.at[step], parts_in.at[step], x_send.at[step], x_recv.at[step], at_x(step))
    for step in orders[:-1]:
        arrived(parts_in.at[step], x_recv.at[step])
    for slot in range(2):
        total = out[slot]
        for step in range(1, x_count):
            total += parts_in[step, slot].astype(jnp.float32)
        s = high * 2 * x_count + 2 * x + slot
        out[slot] = jnp.where(s < c_cnt[0], total, 0.0)
    for copy in sent:
        copy.wait_send()


def on_device(a_values, a_index, a_count, b_values, b_index, b_count, c_index, c_count):
    row_count, col_count = lax.axis_size("row"), lax.axis_size("col")
    x_count = lax.axis_size("layer_1")
    y_count, z_count = row_count // 2, 2 * col_count
    reach = z_count // 2
    block = a_values.shape[-1]
    dtype = a_values.dtype
    smem = pl.BlockSpec(memory_space=pltpu.SMEM)
    anywhere = pl.BlockSpec(memory_space=pl.ANY)
    vmem = pl.BlockSpec(memory_space=pltpu.VMEM)
    result = pl.pallas_call(
        functools.partial(kernel, (row_count, col_count, x_count)),
        out_shape=jax.ShapeDtypeStruct((2, block, block), jnp.float32),
        in_specs=[smem] * 6 + [anywhere] * 2,
        out_specs=vmem,
        scratch_shapes=[
            pltpu.VMEM((2 * z_count, block, block), dtype),
            pltpu.VMEM((z_count, 1, 128), jnp.int32),
            pltpu.SMEM((z_count, 1, 128), jnp.int32),
            pltpu.VMEM((2 * row_count, block, block), dtype),
            pltpu.VMEM((row_count, 1, 128), jnp.int32),
            pltpu.SMEM((row_count, 1, 128), jnp.int32),
            pltpu.VMEM((2, reach, block // 2, block), dtype),
            pltpu.VMEM((row_count, block, block), dtype),
            pltpu.VMEM((x_count, 2, block, block), dtype),
            pltpu.VMEM((x_count, 2, block, block), dtype),
            pltpu.SemaphoreType.DMA((4,)),
            pltpu.SemaphoreType.DMA((2, 2 * reach)),
            pltpu.SemaphoreType.DMA((2, 2 * reach)),
            pltpu.SemaphoreType.DMA((2, reach)),
            pltpu.SemaphoreType.DMA((2, reach)),
            pltpu.SemaphoreType.DMA((3, y_count)),
            pltpu.SemaphoreType.DMA((3, y_count)),
            pltpu.SemaphoreType.DMA((3, y_count)),
            pltpu.SemaphoreType.DMA((3, y_count)),
            pltpu.SemaphoreType.DMA((2, reach)),
            pltpu.SemaphoreType.DMA((2, reach)),
            pltpu.SemaphoreType.DMA((x_count,)),
            pltpu.SemaphoreType.DMA((x_count,)),
        ],
        compiler_params=pltpu.CompilerParams(
            collective_id=0, has_side_effects=True, vmem_limit_bytes=40 * 1024 * 1024
        ),
    )(
        a_index[0, 0, 0].reshape(-1),
        a_count[0, 0],
        b_index[0, 0, 0].reshape(-1),
        b_count[0, 0],
        c_index[0, 0],
        c_count[0],
        a_values[0, 0, 0],
        b_values[0, 0, 0].transpose(1, 0, 2),
    )
    return result[None, None]


def solution(mesh):
    highs = 2
    split = Mesh(
        mesh.devices.reshape(mesh.shape["row"], mesh.shape["col"], highs, mesh.shape["layer"] // highs),
        ("row", "col", "layer_0", "layer_1"),
    )
    return jax.shard_map(
        on_device,
        mesh=split,
        in_specs=(
            P("row", LAYER, "col", None, None, None),
            P("row", LAYER, "col", None, None),
            P("row", LAYER, "col"),
            P(LAYER, "row", "col", None, None, None),
            P(LAYER, "row", "col", None, None),
            P(LAYER, "row", "col"),
            P("row", "col", None, None),
            P("row", "col"),
        ),
        out_specs=P("row", "col", LAYER, None, None),
        check_vma=False,
    )
```

```python
import functools

import jax
import jax.numpy as jnp
from jax import lax
from jax.experimental import pallas as pl
from jax.experimental.pallas import tpu as pltpu
from jax.sharding import Mesh
from jax.sharding import PartitionSpec as P

LAYER = ("layer_0", "layer_1")
MESH = pl.DeviceIdType.MESH
LINKS, RING, LISTS = 40, 12, 6
B_PASS, B_CORES, B_TURN, B_WAY, B_FAR, B_FAR_PASS, B_FAR_CORES, B_FAR_DONE = 4, 7, 9, 14, 19, 22, 25, 27


def kernel(
    sizes,
    a_idx_in,
    a_cnt_in,
    b_idx_in,
    b_cnt_in,
    c_idx_in,
    c_cnt_in,
    a_in,
    b_in,
    out,
    a_idx,
    a_cnt,
    b_idx,
    b_cnt,
    c_idx,
    c_cnt,
    b_raw,
    a_all,
    a_meta,
    a_tab,
    b_all,
    b_meta,
    b_tab,
    b_hop,
    b_far,
    kept,
    parts_out,
    parts_in,
    local_sem,
    send_sem,
    recv_sem,
    ring_send,
    ring_recv,
    list_send,
    list_recv,
):
    row_count, col_count, x_count = sizes
    y_count = row_count // 2
    z_count = 2 * col_count
    reach = z_count // 2
    stride = reach // 2
    half = a_in.shape[1] // 2
    row, col = lax.axis_index("row"), lax.axis_index("col")
    high, x = lax.axis_index("layer_0"), lax.axis_index("layer_1")
    y, core = row // 2, row % 2
    z = high * col_count + col

    def at_z(step):
        there = (z + step + z_count) % z_count
        return {"layer_0": there // col_count, "col": there % col_count}

    def row_at(step, which):
        return ((y + step + y_count) % y_count) * 2 + which

    def at_row(step, which):
        return {"row": row_at(step, which)}

    def at_x(step):
        return {"layer_1": (x + step + x_count) % x_count}

    sent = []

    def send(src, dst, where):
        link = len(sent)
        copy = pltpu.make_async_remote_copy(
            src_ref=src,
            dst_ref=dst,
            send_sem=send_sem.at[link],
            recv_sem=recv_sem.at[link],
            device_id=where,
            device_id_type=MESH,
        )
        copy.start()
        sent.append(copy)
        return link

    def arrived(ref, link):
        pltpu.make_async_copy(ref, ref, recv_sem.at[link]).wait()

    def ring_copy(src, dst, sends, recvs, place, side):
        return pltpu.make_async_remote_copy(
            src_ref=src,
            dst_ref=dst,
            send_sem=sends.at[place],
            recv_sem=recvs.at[place],
            device_id=at_z(1 - 2 * side),
            device_id_type=MESH,
        )

    def ring_send_on(flying, copy, place):
        if place in flying:
            flying[place].wait_send()
        copy.start()
        flying[place] = copy

    def ring_arrived(ref, recvs, place):
        pltpu.make_async_copy(ref, ref, recvs.at[place]).wait()

    loads = [
        pltpu.make_async_copy(src, dst, local_sem.at[n])
        for n, (src, dst) in enumerate(
            (
                (a_in, a_all.at[pl.ds(0, 2)]),
                (a_idx_in, a_idx),
                (a_cnt_in, a_cnt),
                (b_idx_in, b_idx),
                (b_cnt_in, b_cnt),
                (c_idx_in, c_idx),
                (c_cnt_in, c_cnt),
                (b_in, b_raw),
            )
        )
    ]
    for load in loads:
        load.start()
    barrier = pltpu.get_barrier_semaphore()
    partners = [at_z(1), at_z(-1), at_row(0, 1 - core), at_row(1, core), at_row(-1, core), at_x(1), at_x(-1)]
    for partner in partners:
        pl.semaphore_signal(barrier, inc=1, device_id=partner, device_id_type=MESH)
    for load in loads[:-1]:
        load.wait()
    lane = lax.broadcasted_iota(jnp.int32, (1, 128), 1)
    listed = jnp.zeros((1, 128), jnp.int32)
    for place, value in enumerate((a_idx[0, 0], a_idx[0, 1], a_cnt[0, 0], b_idx[1, 0], b_idx[1, 1], b_cnt[0, 0])):
        listed = jnp.where(lane == place, value, listed)
    a_meta[0] = listed
    b_meta[row] = listed
    pl.semaphore_wait(barrier, len(partners))

    a_left, a_flying = set(), {}

    def a_slot(side, tick):
        step, slot = tick // 2, tick % 2
        if step == reach - 1:
            slot = side
        offset = (z_count - step) % z_count if side == 0 else step
        beyond = z_count - step - 1 if side == 0 else step + 1
        return 2 * offset + slot, 2 * beyond + slot

    def a_place(side, tick, part):
        return side * RING + (2 * tick + part) % RING

    def a_tick(tick):
        for part in range(2):
            rows = pl.ds(part * half, half)
            for side in range(2):
                here, there = a_slot(side, tick)
                if tick >= 2:
                    before = tick - 2
                    if tick // 2 == reach - 1:
                        before = tick - 2 + side
                    ring_arrived(a_all.at[here, rows], ring_recv, a_place(side, before, part))
                    a_left.remove((side, before, part))
                place = a_place(side, tick, part)
                copy = ring_copy(a_all.at[here, rows], a_all.at[there, rows], ring_send, ring_recv, place, side)
                ring_send_on(a_flying, copy, place)
                a_left.add((side, tick, part))

    def a_done():
        for side, tick, part in sorted(a_left):
            block = a_all.at[a_slot(side, tick)[1], pl.ds(part * half, half)]
            ring_arrived(block, ring_recv, a_place(side, tick, part))

    lists_flying = {}

    def lists_step(step):
        for side in range(2):
            offset = (z_count - step) % z_count if side == 0 else step
            beyond = z_count - step - 1 if side == 0 else step + 1
            if step >= 1:
                ring_arrived(a_meta.at[offset], list_recv, side * LISTS + (step - 1) % LISTS)
            if step < reach - 1 + (side == 0):
                place = side * LISTS + step % LISTS
                copy = ring_copy(a_meta.at[offset], a_meta.at[beyond], list_send, list_recv, place, side)
                ring_send_on(lists_flying, copy, place)

    def lists_done():
        ring_arrived(a_meta.at[reach], list_recv, (reach - 1) % LISTS)
        table = pltpu.make_async_copy(a_meta, a_tab, local_sem.at[8])
        table.start()
        table.wait()

    def tile_from(step, which):
        return b_all.at[pl.ds(2 * row_at(step, which), 2)]

    def lists_from(step, which):
        return b_meta.at[row_at(step, which)]

    def slot_from(step, which, slot):
        return b_all.at[2 * row_at(step, which) + slot]

    b_links = {}

    def b_over_y():
        loads[-1].wait()
        for slot in range(2):
            b_all[2 * row + slot] = b_raw[:, slot, :]
        tile, lists = tile_from(0, core), lists_from(0, core)
        for step in (1, -1):
            b_links["lists", step] = send(lists, lists, at_row(step, core))
            b_links["tile", step] = send(tile, tile, at_row(step, core))
        b_links["lists", "d", 0] = send(lists, lists, at_row(0, 1 - core))
        b_links["tile", "d", 0] = send(tile, tile, at_row(0, 1 - core))

    def b_pass():
        for step in (1, -1):
            slot = 0 if step == 1 else 1
            tile, lists = tile_from(-step, core), lists_from(-step, core)
            arrived(lists, b_links["lists", step])
            arrived(tile, b_links["tile", step])
            one = slot_from(-step, core, slot)
            b_links["one", step] = send(one, one, at_row(step, core))
            if step == 1:
                b_links["lists", 2] = send(lists, lists, at_row(step, core))
            b_links["lists", "d", -step] = send(lists, lists, at_row(0, 1 - core))
            b_links["tile", "d", -step] = send(tile, tile, at_row(0, 1 - core))

    def b_cores():
        tile, lists = tile_from(2, core), lists_from(2, core)
        arrived(lists, b_links["lists", 2])
        for step in (1, -1):
            arrived(slot_from(2, core, 0 if step == 1 else 1), b_links["one", step])
        b_links["lists", "d", 2] = send(lists, lists, at_row(0, 1 - core))
        b_links["tile", "d", 2] = send(tile, tile, at_row(0, 1 - core))

    def place_of_b(column):
        place = jnp.int32(0)
        for r in range(row_count):
            for slot in range(2):
                hit = (b_tab[r, 0, 3 + slot] == column) & (slot < b_tab[r, 0, 5])
                place = jnp.where(hit, 2 * r + slot, place)
        return place

    def b_turn():
        for step in (0, 1, -1, 2):
            arrived(lists_from(step, 1 - core), b_links["lists", "d", step])
            arrived(tile_from(step, 1 - core), b_links["tile", "d", step])
        table = pltpu.make_async_copy(b_meta, b_tab, local_sem.at[9])
        table.start()
        table.wait()
        block = b_all[place_of_b(row)]
        for side in range(2):
            b_hop[side, 0] = block[side * half : (side + 1) * half]
        for side in range(2):
            b_links["way", side] = send(b_hop.at[side, 0], b_hop.at[side, 1], at_z(stride * (1 - 2 * side)))

    def far_half(step, which, side):
        return b_far.at[row_at(step, which), pl.ds(side * half, half)]

    def b_way():
        for side in range(2):
            arrived(b_hop.at[side, 1], b_links["way", side])
            b_links["far", side] = send(
                b_hop.at[side, 1], far_half(0, core, side), at_z((reach - stride) * (1 - 2 * side))
            )

    def b_far_over_y():
        block = b_far.at[row]
        for side in range(2):
            arrived(far_half(0, core, side), b_links["far", side])
        for step in (1, -1):
            b_links["block", step] = send(block, block, at_row(step, core))
        b_links["block", "d", 0] = send(block, block, at_row(0, 1 - core))

    def b_far_pass():
        for step in (1, -1):
            block, one = b_far.at[row_at(-step, core)], far_half(-step, core, 0 if step == 1 else 1)
            arrived(block, b_links["block", step])
            b_links["part", step] = send(one, one, at_row(step, core))
            b_links["block", "d", -step] = send(block, block, at_row(0, 1 - core))

    def b_far_cores():
        for step in (1, -1):
            arrived(far_half(2, core, 0 if step == 1 else 1), b_links["part", step])
        block = b_far.at[row_at(2, core)]
        b_links["block", "d", 2] = send(block, block, at_row(0, 1 - core))

    def b_far_done():
        for step in (0, 1, -1, 2):
            arrived(b_far.at[row_at(step, 1 - core)], b_links["block", "d", step])

    wanted = {}

    def find_blocks():
        slots = []
        for step in range(x_count):
            for slot in range(2):
                s = high * 2 * x_count + 2 * ((x + step) % x_count) + slot
                slots.append((step, slot, c_idx[0, s], c_idx[1, s]))

        def look(o, places):
            other = ((z + o) % z_count) // col_count != high
            places = list(places)
            for which in range(2):
                found = a_tab[o, 0, which]
                live = which < a_tab[o, 0, 2]
                here = 2 * o + which
                for n, (_, _, i, _) in enumerate(slots):
                    hit = live & (found == i)
                    places[2 * n] = jnp.where(hit & jnp.logical_not(other), here, places[2 * n])
                    places[2 * n + 1] = jnp.where(hit & other, here, places[2 * n + 1])
            return tuple(places)

        places = lax.fori_loop(0, z_count, look, (jnp.int32(0),) * (2 * len(slots)))
        for n, (step, slot, _, j) in enumerate(slots):
            wanted[step, slot] = (places[2 * n], places[2 * n + 1], place_of_b(j), j)

    def product(step, slot):
        near, far, b_near, j = wanted[step, slot]
        total = jnp.dot(a_all[near], b_all[b_near], preferred_element_type=jnp.float32)
        return total + jnp.dot(a_all[far], b_far[j], preferred_element_type=jnp.float32)

    stages = [(0, b_over_y), (B_PASS, b_pass), (B_CORES, b_cores), (B_TURN, b_turn), (B_WAY, b_way)]
    stages += [(B_FAR, b_far_over_y), (B_FAR_PASS, b_far_pass), (B_FAR_CORES, b_far_cores), (B_FAR_DONE, b_far_done)]
    stages += [(step, functools.partial(lists_step, step)) for step in range(reach)]
    stages += [(B_TURN + reach, lists_done), (B_TURN + reach + 1, find_blocks)]
    stages.sort(key=lambda pair: pair[0])
    for tick in range(2 * reach - 1):
        a_tick(tick)
        while stages and stages[0][0] <= tick:
            stages.pop(0)[1]()
    for _, stage in stages:
        stage()
    a_done()

    def pass_on(n, value, step):
        parts_out[n] = value.astype(jnp.bfloat16)
        return send(parts_out.at[n], parts_in.at[n], at_x(step))

    def taken(n, link):
        arrived(parts_in.at[n], link)
        return parts_in[n].astype(jnp.float32)

    up = pass_on(0, product(2, 0), 1)
    down = pass_on(1, product(2, 1), -1)
    below = pass_on(2, product(1, 1), 1)
    above = pass_on(3, product(3, 0), -1)
    kept[0] = product(1, 0)
    kept[1] = product(3, 1)
    out[0] = product(0, 0)
    out[1] = product(0, 1)
    up = pass_on(4, kept[0] + taken(0, up), 1)
    down = pass_on(5, kept[1] + taken(1, down), -1)
    out[1] += taken(2, below)
    out[0] += taken(3, above)
    for slot, (n, link) in enumerate(((4, up), (5, down))):
        s = high * 2 * x_count + 2 * x + slot
        out[slot] = jnp.where(s < c_cnt[0, 0], out[slot] + taken(n, link), 0.0)
    for copy in [*sent, *a_flying.values(), *lists_flying.values()]:
        copy.wait_send()


def on_device(a_values, a_index, a_count, b_values, b_index, b_count, c_index, c_count):
    row_count, col_count = lax.axis_size("row"), lax.axis_size("col")
    x_count = lax.axis_size("layer_1")
    assert row_count == 8 and x_count == 4
    z_count = 2 * col_count
    block = a_values.shape[-1]
    dtype = a_values.dtype
    far_memory = pl.BlockSpec(memory_space=pltpu.HBM)
    vmem = pl.BlockSpec(memory_space=pltpu.VMEM)
    lists = (
        a_index[0, 0, 0],
        a_count[0, 0][None],
        b_index[0, 0, 0],
        b_count[0, 0][None],
        c_index[0, 0],
        c_count,
    )
    result = pl.pallas_call(
        functools.partial(kernel, (row_count, col_count, x_count)),
        out_shape=jax.ShapeDtypeStruct((2, block, block), jnp.float32),
        in_specs=[far_memory] * 8,
        out_specs=vmem,
        scratch_shapes=[pltpu.SMEM(x.shape, jnp.int32) for x in lists]
        + [
            pltpu.VMEM((block, 2, block), dtype),
            pltpu.VMEM((2 * z_count, block, block), dtype),
            pltpu.VMEM((z_count, 1, 128), jnp.int32),
            pltpu.SMEM((z_count, 1, 128), jnp.int32),
            pltpu.VMEM((2 * row_count, block, block), dtype),
            pltpu.VMEM((row_count, 1, 128), jnp.int32),
            pltpu.SMEM((row_count, 1, 128), jnp.int32),
            pltpu.VMEM((2, 2, block // 2, block), dtype),
            pltpu.VMEM((row_count, block, block), dtype),
            pltpu.VMEM((2, block, block), jnp.float32),
            pltpu.VMEM((6, block, block), dtype),
            pltpu.VMEM((6, block, block), dtype),
            pltpu.SemaphoreType.DMA((10,)),
            pltpu.SemaphoreType.DMA((LINKS,)),
            pltpu.SemaphoreType.DMA((LINKS,)),
            pltpu.SemaphoreType.DMA((2 * RING,)),
            pltpu.SemaphoreType.DMA((2 * RING,)),
            pltpu.SemaphoreType.DMA((2 * LISTS,)),
            pltpu.SemaphoreType.DMA((2 * LISTS,)),
        ],
        compiler_params=pltpu.CompilerParams(
            collective_id=0, has_side_effects=True, vmem_limit_bytes=40 * 1024 * 1024
        ),
    )(*lists, a_values[0, 0, 0], b_values[0, 0, 0])
    return result[None, None]


def solution(mesh):
    highs = 2
    split = Mesh(
        mesh.devices.reshape(mesh.shape["row"], mesh.shape["col"], highs, mesh.shape["layer"] // highs),
        ("row", "col", "layer_0", "layer_1"),
    )
    return jax.shard_map(
        on_device,
        mesh=split,
        in_specs=(
            P("row", LAYER, "col", None, None, None),
            P("row", LAYER, "col", None, None),
            P("row", LAYER, "col"),
            P(LAYER, "row", "col", None, None, None),
            P(LAYER, "row", "col", None, None),
            P(LAYER, "row", "col"),
            P("row", "col", None, None),
            P("row", "col"),
        ),
        out_specs=P("row", "col", LAYER, None, None),
        check_vma=False,
    )
```

```python
import functools

import jax
import jax.numpy as jnp
from jax import lax
from jax.experimental import pallas as pl
from jax.experimental.pallas import tpu as pltpu
from jax.sharding import Mesh
from jax.sharding import PartitionSpec as P

LAYER = ("layer_0", "layer_1")
MESH = pl.DeviceIdType.MESH
LINKS, RING, LISTS = 48, 12, 6
B_PASS, B_CORES, B_TURN, B_WAY, B_FAR, B_FAR_PASS, B_FAR_CORES, B_FAR_DONE = 4, 7, 9, 14, 19, 22, 25, 27


def kernel(
    sizes,
    a_idx_in,
    a_cnt_in,
    b_idx_in,
    b_cnt_in,
    c_idx_in,
    c_cnt_in,
    a_in,
    b_in,
    out,
    a_idx,
    a_cnt,
    b_idx,
    b_cnt,
    c_idx,
    c_cnt,
    b_raw,
    a_all,
    a_meta,
    a_tab,
    b_all,
    b_meta,
    b_tab,
    b_hop,
    b_far,
    kept,
    parts_out,
    parts_in,
    local_sem,
    send_sem,
    recv_sem,
    ring_send,
    ring_recv,
    list_send,
    list_recv,
):
    row_count, col_count, x_count = sizes
    y_count = row_count // 2
    z_count = 2 * col_count
    reach = z_count // 2
    stride = reach // 2
    half = a_in.shape[1] // 2
    row, col = lax.axis_index("row"), lax.axis_index("col")
    high, x = lax.axis_index("layer_0"), lax.axis_index("layer_1")
    y, core = row // 2, row % 2
    z = high * col_count + col

    def at_z(step):
        there = (z + step + z_count) % z_count
        return {"layer_0": there // col_count, "col": there % col_count}

    def row_at(step, which):
        return ((y + step + y_count) % y_count) * 2 + which

    def at_row(step, which):
        return {"row": row_at(step, which)}

    def at_x(step):
        return {"layer_1": (x + step + x_count) % x_count}

    sent = []

    def send(src, dst, where):
        link = len(sent)
        copy = pltpu.make_async_remote_copy(
            src_ref=src,
            dst_ref=dst,
            send_sem=send_sem.at[link],
            recv_sem=recv_sem.at[link],
            device_id=where,
            device_id_type=MESH,
        )
        copy.start()
        sent.append(copy)
        return link

    def arrived(ref, link):
        pltpu.make_async_copy(ref, ref, recv_sem.at[link]).wait()

    def ring_copy(src, dst, sends, recvs, place, side):
        return pltpu.make_async_remote_copy(
            src_ref=src,
            dst_ref=dst,
            send_sem=sends.at[place],
            recv_sem=recvs.at[place],
            device_id=at_z(1 - 2 * side),
            device_id_type=MESH,
        )

    def ring_send_on(flying, copy, place):
        if place in flying:
            flying[place].wait_send()
        copy.start()
        flying[place] = copy

    def ring_arrived(ref, recvs, place):
        pltpu.make_async_copy(ref, ref, recvs.at[place]).wait()

    loads = [
        pltpu.make_async_copy(src, dst, local_sem.at[n])
        for n, (src, dst) in enumerate(
            (
                (a_in, a_all.at[pl.ds(0, 2)]),
                (a_idx_in, a_idx),
                (a_cnt_in, a_cnt),
                (b_idx_in, b_idx),
                (b_cnt_in, b_cnt),
                (c_idx_in, c_idx),
                (c_cnt_in, c_cnt),
                (b_in, b_raw),
            )
        )
    ]
    for load in loads:
        load.start()
    barrier = pltpu.get_barrier_semaphore()
    partners = [at_z(1), at_z(-1), at_row(0, 1 - core), at_row(1, core), at_row(-1, core), at_x(1), at_x(-1)]
    for partner in partners:
        pl.semaphore_signal(barrier, inc=1, device_id=partner, device_id_type=MESH)
    for load in loads[:-1]:
        load.wait()
    lane = lax.broadcasted_iota(jnp.int32, (1, 128), 1)
    listed = jnp.zeros((1, 128), jnp.int32)
    for place, value in enumerate((a_idx[0, 0], a_idx[0, 1], a_cnt[0, 0], b_idx[1, 0], b_idx[1, 1], b_cnt[0, 0])):
        listed = jnp.where(lane == place, value, listed)
    a_meta[0] = listed
    b_meta[row] = listed
    pl.semaphore_wait(barrier, len(partners))

    a_left, a_flying = set(), {}

    def a_slot(side, tick):
        step, slot = tick // 2, tick % 2
        if step == reach - 1:
            slot = side
        offset = (z_count - step) % z_count if side == 0 else step
        beyond = z_count - step - 1 if side == 0 else step + 1
        return 2 * offset + slot, 2 * beyond + slot

    def a_place(side, tick, part):
        return side * RING + (2 * tick + part) % RING

    def a_tick(tick):
        for part in range(2):
            rows = pl.ds(part * half, half)
            for side in range(2):
                here, there = a_slot(side, tick)
                if tick >= 2:
                    before = tick - 2
                    if tick // 2 == reach - 1:
                        before = tick - 2 + side
                    ring_arrived(a_all.at[here, rows], ring_recv, a_place(side, before, part))
                    a_left.remove((side, before, part))
                place = a_place(side, tick, part)
                copy = ring_copy(a_all.at[here, rows], a_all.at[there, rows], ring_send, ring_recv, place, side)
                ring_send_on(a_flying, copy, place)
                a_left.add((side, tick, part))

    def a_done():
        for side, tick, part in sorted(a_left):
            block = a_all.at[a_slot(side, tick)[1], pl.ds(part * half, half)]
            ring_arrived(block, ring_recv, a_place(side, tick, part))

    lists_flying = {}

    def lists_step(step):
        for side in range(2):
            offset = (z_count - step) % z_count if side == 0 else step
            beyond = z_count - step - 1 if side == 0 else step + 1
            if step >= 1:
                ring_arrived(a_meta.at[offset], list_recv, side * LISTS + (step - 1) % LISTS)
            if step < reach - 1 + (side == 0):
                place = side * LISTS + step % LISTS
                copy = ring_copy(a_meta.at[offset], a_meta.at[beyond], list_send, list_recv, place, side)
                ring_send_on(lists_flying, copy, place)

    def lists_done():
        ring_arrived(a_meta.at[reach], list_recv, (reach - 1) % LISTS)
        table = pltpu.make_async_copy(a_meta, a_tab, local_sem.at[8])
        table.start()
        table.wait()

    def tile_from(step, which):
        return b_all.at[pl.ds(2 * row_at(step, which), 2)]

    def lists_from(step, which):
        return b_meta.at[row_at(step, which)]

    def slot_from(step, which, slot):
        return b_all.at[2 * row_at(step, which) + slot]

    b_links = {}

    def b_over_y():
        loads[-1].wait()
        for slot in range(2):
            b_all[2 * row + slot] = b_raw[:, slot, :]
        tile, lists = tile_from(0, core), lists_from(0, core)
        for step in (1, -1):
            b_links["lists", step] = send(lists, lists, at_row(step, core))
            b_links["tile", step] = send(tile, tile, at_row(step, core))
        b_links["lists", "d", 0] = send(lists, lists, at_row(0, 1 - core))
        b_links["tile", "d", 0] = send(tile, tile, at_row(0, 1 - core))

    def b_pass():
        for step in (1, -1):
            slot = 0 if step == 1 else 1
            tile, lists = tile_from(-step, core), lists_from(-step, core)
            arrived(lists, b_links["lists", step])
            arrived(tile, b_links["tile", step])
            one = slot_from(-step, core, slot)
            b_links["one", step] = send(one, one, at_row(step, core))
            if step == 1:
                b_links["lists", 2] = send(lists, lists, at_row(step, core))
            b_links["lists", "d", -step] = send(lists, lists, at_row(0, 1 - core))
            b_links["tile", "d", -step] = send(tile, tile, at_row(0, 1 - core))

    def b_cores():
        tile, lists = tile_from(2, core), lists_from(2, core)
        arrived(lists, b_links["lists", 2])
        for step in (1, -1):
            arrived(slot_from(2, core, 0 if step == 1 else 1), b_links["one", step])
        b_links["lists", "d", 2] = send(lists, lists, at_row(0, 1 - core))
        b_links["tile", "d", 2] = send(tile, tile, at_row(0, 1 - core))

    def place_of_b(column):
        place = jnp.int32(0)
        for r in range(row_count):
            for slot in range(2):
                hit = (b_tab[r, 0, 3 + slot] == column) & (slot < b_tab[r, 0, 5])
                place = jnp.where(hit, 2 * r + slot, place)
        return place

    third = 3 * a_in.shape[1] // 8
    up_rows, down_rows = pl.ds(0, third), pl.ds(third, third)
    mid_rows = pl.ds(2 * third, a_in.shape[1] - 2 * third)
    relays = (z >= stride) & (z < 3 * stride)
    mid_send, mid_up, mid_down, relay_up, relay_down, mid_far = range(LINKS - 6, LINKS)

    def mid_copy(src, dst, step, send_link, recv_link):
        return pltpu.make_async_remote_copy(
            src_ref=src,
            dst_ref=dst,
            send_sem=send_sem.at[send_link],
            recv_sem=recv_sem.at[recv_link],
            device_id=at_z(step),
            device_id_type=MESH,
        )

    def mid_relays():
        return (
            mid_copy(b_hop.at[1, mid_rows], b_far.at[row, mid_rows], reach - stride, relay_up, mid_far),
            mid_copy(b_hop.at[2, mid_rows], b_far.at[row, mid_rows], stride - reach, relay_down, mid_far),
        )

    def b_turn():
        for step in (0, 1, -1, 2):
            arrived(lists_from(step, 1 - core), b_links["lists", "d", step])
            arrived(tile_from(step, 1 - core), b_links["tile", "d", step])
        table = pltpu.make_async_copy(b_meta, b_tab, local_sem.at[9])
        table.start()
        table.wait()
        b_hop[0] = b_all[place_of_b(row)]
        b_links["way", 0] = send(b_hop.at[0, up_rows], b_hop.at[1, up_rows], at_z(stride))
        b_links["way", 1] = send(b_hop.at[0, down_rows], b_hop.at[1, down_rows], at_z(-stride))

        @pl.when(high == 0)
        def _():
            mid_copy(b_hop.at[0, mid_rows], b_hop.at[1, mid_rows], stride, mid_send, mid_up).start()

        @pl.when(high == 1)
        def _():
            mid_copy(b_hop.at[0, mid_rows], b_hop.at[2, mid_rows], -stride, mid_send, mid_down).start()

    def far_half(step, which, side):
        return b_far.at[row_at(step, which), pl.ds(side * half, half)]

    def b_way():
        for side, rows in enumerate((up_rows, down_rows)):
            arrived(b_hop.at[1, rows], b_links["way", side])
            step = (reach - stride) * (1 - 2 * side)
            b_links["far", side] = send(b_hop.at[1, rows], b_far.at[row, rows], at_z(step))

        @pl.when(relays)
        def _():
            arrived(b_hop.at[1, mid_rows], mid_up)
            arrived(b_hop.at[2, mid_rows], mid_down)
            for copy in mid_relays():
                copy.start()

    def b_far_over_y():
        block = b_far.at[row]
        for side, rows in enumerate((up_rows, down_rows)):
            arrived(b_far.at[row, rows], b_links["far", side])
        arrived(b_far.at[row, mid_rows], mid_far)
        for step in (1, -1):
            b_links["block", step] = send(block, block, at_row(step, core))
        b_links["block", "d", 0] = send(block, block, at_row(0, 1 - core))

    def b_far_pass():
        for step in (1, -1):
            block, one = b_far.at[row_at(-step, core)], far_half(-step, core, 0 if step == 1 else 1)
            arrived(block, b_links["block", step])
            b_links["part", step] = send(one, one, at_row(step, core))
            b_links["block", "d", -step] = send(block, block, at_row(0, 1 - core))

    def b_far_cores():
        for step in (1, -1):
            arrived(far_half(2, core, 0 if step == 1 else 1), b_links["part", step])
        block = b_far.at[row_at(2, core)]
        b_links["block", "d", 2] = send(block, block, at_row(0, 1 - core))

    def b_far_done():
        for step in (0, 1, -1, 2):
            arrived(b_far.at[row_at(step, 1 - core)], b_links["block", "d", step])

    wanted = {}

    def find_blocks():
        slots = []
        for step in range(x_count):
            for slot in range(2):
                s = high * 2 * x_count + 2 * ((x + step) % x_count) + slot
                slots.append((step, slot, c_idx[0, s], c_idx[1, s]))

        def look(o, places):
            other = ((z + o) % z_count) // col_count != high
            places = list(places)
            for which in range(2):
                found = a_tab[o, 0, which]
                live = which < a_tab[o, 0, 2]
                here = 2 * o + which
                for n, (_, _, i, _) in enumerate(slots):
                    hit = live & (found == i)
                    places[2 * n] = jnp.where(hit & jnp.logical_not(other), here, places[2 * n])
                    places[2 * n + 1] = jnp.where(hit & other, here, places[2 * n + 1])
            return tuple(places)

        places = lax.fori_loop(0, z_count, look, (jnp.int32(0),) * (2 * len(slots)))
        for n, (step, slot, _, j) in enumerate(slots):
            wanted[step, slot] = (places[2 * n], places[2 * n + 1], place_of_b(j), j)

    def product(step, slot):
        near, far, b_near, j = wanted[step, slot]
        total = jnp.dot(a_all[near], b_all[b_near], preferred_element_type=jnp.float32)
        return total + jnp.dot(a_all[far], b_far[j], preferred_element_type=jnp.float32)

    stages = [(0, b_over_y), (B_PASS, b_pass), (B_CORES, b_cores), (B_TURN, b_turn), (B_WAY, b_way)]
    stages += [(B_FAR, b_far_over_y), (B_FAR_PASS, b_far_pass), (B_FAR_CORES, b_far_cores), (B_FAR_DONE, b_far_done)]
    stages += [(step, functools.partial(lists_step, step)) for step in range(reach)]
    stages += [(B_TURN + reach, lists_done), (B_TURN + reach + 1, find_blocks)]
    stages.sort(key=lambda pair: pair[0])
    for tick in range(2 * reach - 1):
        a_tick(tick)
        while stages and stages[0][0] <= tick:
            stages.pop(0)[1]()
    for _, stage in stages:
        stage()
    a_done()

    def pass_on(n, value, step):
        parts_out[n] = value.astype(jnp.bfloat16)
        return send(parts_out.at[n], parts_in.at[n], at_x(step))

    def taken(n, link):
        arrived(parts_in.at[n], link)
        return parts_in[n].astype(jnp.float32)

    up = pass_on(0, product(2, 0), 1)
    down = pass_on(1, product(2, 1), -1)
    below = pass_on(2, product(1, 1), 1)
    above = pass_on(3, product(3, 0), -1)
    kept[0] = product(1, 0)
    kept[1] = product(3, 1)
    out[0] = product(0, 0)
    out[1] = product(0, 1)
    up = pass_on(4, kept[0] + taken(0, up), 1)
    down = pass_on(5, kept[1] + taken(1, down), -1)
    out[1] += taken(2, below)
    out[0] += taken(3, above)
    for slot, (n, link) in enumerate(((4, up), (5, down))):
        s = high * 2 * x_count + 2 * x + slot
        out[slot] = jnp.where(s < c_cnt[0, 0], out[slot] + taken(n, link), 0.0)
    for copy in [*sent, *a_flying.values(), *lists_flying.values()]:
        copy.wait_send()
    mid = b_hop.at[0, mid_rows]
    pltpu.make_async_copy(mid, mid, send_sem.at[mid_send]).wait()

    @pl.when(relays)
    def _():
        for copy in mid_relays():
            copy.wait_send()


def on_device(a_values, a_index, a_count, b_values, b_index, b_count, c_index, c_count):
    row_count, col_count = lax.axis_size("row"), lax.axis_size("col")
    x_count = lax.axis_size("layer_1")
    assert row_count == 8 and x_count == 4
    z_count = 2 * col_count
    block = a_values.shape[-1]
    dtype = a_values.dtype
    far_memory = pl.BlockSpec(memory_space=pltpu.HBM)
    vmem = pl.BlockSpec(memory_space=pltpu.VMEM)
    lists = (
        a_index[0, 0, 0],
        a_count[0, 0][None],
        b_index[0, 0, 0],
        b_count[0, 0][None],
        c_index[0, 0],
        c_count,
    )
    result = pl.pallas_call(
        functools.partial(kernel, (row_count, col_count, x_count)),
        out_shape=jax.ShapeDtypeStruct((2, block, block), jnp.float32),
        in_specs=[far_memory] * 8,
        out_specs=vmem,
        scratch_shapes=[pltpu.SMEM(x.shape, jnp.int32) for x in lists]
        + [
            pltpu.VMEM((block, 2, block), dtype),
            pltpu.VMEM((2 * z_count, block, block), dtype),
            pltpu.VMEM((z_count, 1, 128), jnp.int32),
            pltpu.SMEM((z_count, 1, 128), jnp.int32),
            pltpu.VMEM((2 * row_count, block, block), dtype),
            pltpu.VMEM((row_count, 1, 128), jnp.int32),
            pltpu.SMEM((row_count, 1, 128), jnp.int32),
            pltpu.VMEM((3, block, block), dtype),
            pltpu.VMEM((row_count, block, block), dtype),
            pltpu.VMEM((2, block, block), jnp.float32),
            pltpu.VMEM((6, block, block), dtype),
            pltpu.VMEM((6, block, block), dtype),
            pltpu.SemaphoreType.DMA((10,)),
            pltpu.SemaphoreType.DMA((LINKS,)),
            pltpu.SemaphoreType.DMA((LINKS,)),
            pltpu.SemaphoreType.DMA((2 * RING,)),
            pltpu.SemaphoreType.DMA((2 * RING,)),
            pltpu.SemaphoreType.DMA((2 * LISTS,)),
            pltpu.SemaphoreType.DMA((2 * LISTS,)),
        ],
        compiler_params=pltpu.CompilerParams(
            collective_id=0, has_side_effects=True, vmem_limit_bytes=67043328
        ),
    )(*lists, a_values[0, 0, 0], b_values[0, 0, 0])
    return result[None, None]


def solution(mesh):
    highs = 2
    split = Mesh(
        mesh.devices.reshape(mesh.shape["row"], mesh.shape["col"], highs, mesh.shape["layer"] // highs),
        ("row", "col", "layer_0", "layer_1"),
    )
    return jax.shard_map(
        on_device,
        mesh=split,
        in_specs=(
            P("row", LAYER, "col", None, None, None),
            P("row", LAYER, "col", None, None),
            P("row", LAYER, "col"),
            P(LAYER, "row", "col", None, None, None),
            P(LAYER, "row", "col", None, None),
            P(LAYER, "row", "col"),
            P("row", "col", None, None),
            P("row", "col"),
        ),
        out_specs=P("row", "col", LAYER, None, None),
        check_vma=False,
    )
```

```python
import functools

import jax
import jax.numpy as jnp
from jax import lax
from jax.experimental import pallas as pl
from jax.experimental.pallas import tpu as pltpu
from jax.sharding import Mesh
from jax.sharding import PartitionSpec as P

LAYER = ("layer_0", "layer_1")
MESH = pl.DeviceIdType.MESH
LINKS, RING, LISTS = 48, 12, 6
B_PASS, B_CORES, B_TURN, B_WAY, B_FAR, B_FAR_PASS, B_FAR_CORES, B_FAR_DONE = 4, 7, 9, 14, 19, 22, 25, 27


def kernel(
    sizes,
    a_idx_in,
    a_cnt_in,
    b_idx_in,
    b_cnt_in,
    c_idx_in,
    c_cnt_in,
    a_in,
    b_in,
    out,
    a_idx,
    a_cnt,
    b_idx,
    b_cnt,
    c_idx,
    c_cnt,
    b_raw,
    a_all,
    a_meta,
    a_tab,
    b_all,
    b_meta,
    b_tab,
    b_hop,
    b_far,
    kept,
    parts_out,
    parts_in,
    local_sem,
    send_sem,
    recv_sem,
    ring_send,
    ring_recv,
    list_send,
    list_recv,
):
    row_count, col_count, x_count = sizes
    y_count = row_count // 2
    z_count = 2 * col_count
    reach = z_count // 2
    stride = reach // 2
    half = a_in.shape[1] // 2
    row, col = lax.axis_index("row"), lax.axis_index("col")
    high, x = lax.axis_index("layer_0"), lax.axis_index("layer_1")
    y, core = row // 2, row % 2
    z = high * col_count + col

    def at_z(step):
        there = (z + step + z_count) % z_count
        return {"layer_0": there // col_count, "col": there % col_count}

    def row_at(step, which):
        return ((y + step + y_count) % y_count) * 2 + which

    def at_row(step, which):
        return {"row": row_at(step, which)}

    def at_x(step):
        return {"layer_1": (x + step + x_count) % x_count}

    sent = []

    def send(src, dst, where):
        link = len(sent)
        copy = pltpu.make_async_remote_copy(
            src_ref=src,
            dst_ref=dst,
            send_sem=send_sem.at[link],
            recv_sem=recv_sem.at[link],
            device_id=where,
            device_id_type=MESH,
        )
        copy.start()
        sent.append(copy)
        return link

    def arrived(ref, link):
        pltpu.make_async_copy(ref, ref, recv_sem.at[link]).wait()

    def ring_copy(src, dst, sends, recvs, place, side):
        return pltpu.make_async_remote_copy(
            src_ref=src,
            dst_ref=dst,
            send_sem=sends.at[place],
            recv_sem=recvs.at[place],
            device_id=at_z(1 - 2 * side),
            device_id_type=MESH,
        )

    def ring_send_on(flying, copy, place):
        if place in flying:
            flying[place].wait_send()
        copy.start()
        flying[place] = copy

    def ring_arrived(ref, recvs, place):
        pltpu.make_async_copy(ref, ref, recvs.at[place]).wait()

    loads = [
        pltpu.make_async_copy(src, dst, local_sem.at[n])
        for n, (src, dst) in enumerate(
            (
                (a_in, a_all.at[pl.ds(0, 2)]),
                (a_idx_in, a_idx),
                (a_cnt_in, a_cnt),
                (b_idx_in, b_idx),
                (b_cnt_in, b_cnt),
                (c_idx_in, c_idx),
                (c_cnt_in, c_cnt),
                (b_in, b_raw),
            )
        )
    ]
    for load in loads:
        load.start()
    barrier = pltpu.get_barrier_semaphore()
    partners = [at_z(1), at_z(-1), at_row(0, 1 - core), at_row(1, core), at_row(-1, core), at_x(1), at_x(-1)]
    for partner in partners:
        pl.semaphore_signal(barrier, inc=1, device_id=partner, device_id_type=MESH)
    for load in loads[:-1]:
        load.wait()
    lane = lax.broadcasted_iota(jnp.int32, (1, 128), 1)
    listed = jnp.zeros((1, 128), jnp.int32)
    for place, value in enumerate((a_idx[0, 0], a_idx[0, 1], a_cnt[0, 0], b_idx[1, 0], b_idx[1, 1], b_cnt[0, 0])):
        listed = jnp.where(lane == place, value, listed)
    a_meta[0] = listed
    b_meta[row] = listed
    pl.semaphore_wait(barrier, len(partners))

    a_left, a_flying = set(), {}

    def a_slot(side, tick):
        step, slot = tick // 2, tick % 2
        if step == reach - 1:
            slot = side
        offset = (z_count - step) % z_count if side == 0 else step
        beyond = z_count - step - 1 if side == 0 else step + 1
        return 2 * offset + slot, 2 * beyond + slot

    def a_place(side, tick, part):
        return side * RING + (2 * tick + part) % RING

    def a_tick(tick):
        for part in range(2):
            rows = pl.ds(part * half, half)
            for side in range(2):
                here, there = a_slot(side, tick)
                if tick >= 2:
                    before = tick - 2
                    if tick // 2 == reach - 1:
                        before = tick - 2 + side
                    ring_arrived(a_all.at[here, rows], ring_recv, a_place(side, before, part))
                    a_left.remove((side, before, part))
                place = a_place(side, tick, part)
                copy = ring_copy(a_all.at[here, rows], a_all.at[there, rows], ring_send, ring_recv, place, side)
                ring_send_on(a_flying, copy, place)
                a_left.add((side, tick, part))

    def a_done():
        for side, tick, part in sorted(a_left):
            block = a_all.at[a_slot(side, tick)[1], pl.ds(part * half, half)]
            ring_arrived(block, ring_recv, a_place(side, tick, part))

    lists_flying = {}

    def lists_step(step):
        for side in range(2):
            offset = (z_count - step) % z_count if side == 0 else step
            beyond = z_count - step - 1 if side == 0 else step + 1
            if step >= 1:
                ring_arrived(a_meta.at[offset], list_recv, side * LISTS + (step - 1) % LISTS)
            if step < reach - 1 + (side == 0):
                place = side * LISTS + step % LISTS
                copy = ring_copy(a_meta.at[offset], a_meta.at[beyond], list_send, list_recv, place, side)
                ring_send_on(lists_flying, copy, place)

    def lists_done():
        ring_arrived(a_meta.at[reach], list_recv, (reach - 1) % LISTS)
        table = pltpu.make_async_copy(a_meta, a_tab, local_sem.at[8])
        table.start()
        table.wait()

    def tile_from(step, which):
        return b_all.at[pl.ds(2 * row_at(step, which), 2)]

    def lists_from(step, which):
        return b_meta.at[row_at(step, which)]

    def slot_from(step, which, slot):
        return b_all.at[2 * row_at(step, which) + slot]

    b_links = {}

    def b_over_y():
        loads[-1].wait()
        for slot in range(2):
            b_all[2 * row + slot] = b_raw[:, slot, :]
        tile, lists = tile_from(0, core), lists_from(0, core)
        for step in (1, -1):
            b_links["lists", step] = send(lists, lists, at_row(step, core))
            b_links["tile", step] = send(tile, tile, at_row(step, core))
        b_links["lists", "d", 0] = send(lists, lists, at_row(0, 1 - core))
        b_links["tile", "d", 0] = send(tile, tile, at_row(0, 1 - core))

    def b_pass():
        for step in (1, -1):
            slot = 0 if step == 1 else 1
            tile, lists = tile_from(-step, core), lists_from(-step, core)
            arrived(lists, b_links["lists", step])
            arrived(tile, b_links["tile", step])
            one = slot_from(-step, core, slot)
            b_links["one", step] = send(one, one, at_row(step, core))
            if step == 1:
                b_links["lists", 2] = send(lists, lists, at_row(step, core))
            b_links["lists", "d", -step] = send(lists, lists, at_row(0, 1 - core))
            b_links["tile", "d", -step] = send(tile, tile, at_row(0, 1 - core))

    def b_cores():
        tile, lists = tile_from(2, core), lists_from(2, core)
        arrived(lists, b_links["lists", 2])
        for step in (1, -1):
            arrived(slot_from(2, core, 0 if step == 1 else 1), b_links["one", step])
        b_links["lists", "d", 2] = send(lists, lists, at_row(0, 1 - core))
        b_links["tile", "d", 2] = send(tile, tile, at_row(0, 1 - core))

    def place_of_b(column):
        place = jnp.int32(0)
        for r in range(row_count):
            for slot in range(2):
                hit = (b_tab[r, 0, 3 + slot] == column) & (slot < b_tab[r, 0, 5])
                place = jnp.where(hit, 2 * r + slot, place)
        return place

    third = 3 * a_in.shape[1] // 8
    up_rows, down_rows = pl.ds(0, third), pl.ds(third, third)
    mid_rows = pl.ds(2 * third, a_in.shape[1] - 2 * third)
    relays = (z >= stride) & (z < 3 * stride)
    mid_send, mid_up, mid_down, relay_up, relay_down, mid_far = range(LINKS - 6, LINKS)

    def mid_copy(src, dst, step, send_link, recv_link):
        return pltpu.make_async_remote_copy(
            src_ref=src,
            dst_ref=dst,
            send_sem=send_sem.at[send_link],
            recv_sem=recv_sem.at[recv_link],
            device_id=at_z(step),
            device_id_type=MESH,
        )

    def mid_relays():
        return (
            mid_copy(b_hop.at[1, mid_rows], b_far.at[row, mid_rows], reach - stride, relay_up, mid_far),
            mid_copy(b_hop.at[2, mid_rows], b_far.at[row, mid_rows], stride - reach, relay_down, mid_far),
        )

    def b_turn():
        for step in (0, 1, -1, 2):
            arrived(lists_from(step, 1 - core), b_links["lists", "d", step])
            arrived(tile_from(step, 1 - core), b_links["tile", "d", step])
        table = pltpu.make_async_copy(b_meta, b_tab, local_sem.at[9])
        table.start()
        table.wait()
        b_hop[0] = b_all[place_of_b(row)]
        b_links["way", 0] = send(b_hop.at[0, up_rows], b_hop.at[1, up_rows], at_z(stride))
        b_links["way", 1] = send(b_hop.at[0, down_rows], b_hop.at[1, down_rows], at_z(-stride))

        @pl.when(high == 0)
        def _():
            mid_copy(b_hop.at[0, mid_rows], b_hop.at[1, mid_rows], stride, mid_send, mid_up).start()

        @pl.when(high == 1)
        def _():
            mid_copy(b_hop.at[0, mid_rows], b_hop.at[2, mid_rows], -stride, mid_send, mid_down).start()

    def far_half(step, which, side):
        return b_far.at[row_at(step, which), pl.ds(side * half, half)]

    def b_way():
        for side, rows in enumerate((up_rows, down_rows)):
            arrived(b_hop.at[1, rows], b_links["way", side])
            step = (reach - stride) * (1 - 2 * side)
            b_links["far", side] = send(b_hop.at[1, rows], b_far.at[row, rows], at_z(step))

        @pl.when(relays)
        def _():
            arrived(b_hop.at[1, mid_rows], mid_up)
            arrived(b_hop.at[2, mid_rows], mid_down)
            for copy in mid_relays():
                copy.start()

    def b_far_over_y():
        block = b_far.at[row]
        for side, rows in enumerate((up_rows, down_rows)):
            arrived(b_far.at[row, rows], b_links["far", side])
        arrived(b_far.at[row, mid_rows], mid_far)
        for step in (1, -1):
            b_links["block", step] = send(block, block, at_row(step, core))
        b_links["block", "d", 0] = send(block, block, at_row(0, 1 - core))

    def b_far_pass():
        for step in (1, -1):
            block, one = b_far.at[row_at(-step, core)], far_half(-step, core, 0 if step == 1 else 1)
            arrived(block, b_links["block", step])
            b_links["part", step] = send(one, one, at_row(step, core))
            b_links["block", "d", -step] = send(block, block, at_row(0, 1 - core))

    def b_far_cores():
        for step in (1, -1):
            arrived(far_half(2, core, 0 if step == 1 else 1), b_links["part", step])
        block = b_far.at[row_at(2, core)]
        b_links["block", "d", 2] = send(block, block, at_row(0, 1 - core))

    def b_far_done():
        for step in (0, 1, -1, 2):
            arrived(b_far.at[row_at(step, 1 - core)], b_links["block", "d", step])

    wanted = {}

    def find_blocks():
        slots = []
        for step in range(x_count):
            for slot in range(2):
                s = high * 2 * x_count + 2 * ((x + step) % x_count) + slot
                slots.append((step, slot, c_idx[0, s], c_idx[1, s]))

        def look(o, places):
            other = ((z + o) % z_count) // col_count != high
            places = list(places)
            for which in range(2):
                found = a_tab[o, 0, which]
                live = which < a_tab[o, 0, 2]
                here = 2 * o + which
                for n, (_, _, i, _) in enumerate(slots):
                    hit = live & (found == i)
                    places[2 * n] = jnp.where(hit & jnp.logical_not(other), here, places[2 * n])
                    places[2 * n + 1] = jnp.where(hit & other, here, places[2 * n + 1])
            return tuple(places)

        places = lax.fori_loop(0, z_count, look, (jnp.int32(0),) * (2 * len(slots)))
        for n, (step, slot, _, j) in enumerate(slots):
            wanted[step, slot] = (places[2 * n], places[2 * n + 1], place_of_b(j), j)

    def product(step, slot):
        near, far, b_near, j = wanted[step, slot]
        total = jnp.dot(a_all[near], b_all[b_near], preferred_element_type=jnp.float32)
        return total + jnp.dot(a_all[far], b_far[j], preferred_element_type=jnp.float32)

    stages = [(0, b_over_y), (B_PASS, b_pass), (B_CORES, b_cores), (B_TURN, b_turn), (B_WAY, b_way)]
    stages += [(B_FAR, b_far_over_y), (B_FAR_PASS, b_far_pass), (B_FAR_CORES, b_far_cores), (B_FAR_DONE, b_far_done)]
    stages += [(step, functools.partial(lists_step, step)) for step in range(reach)]
    stages += [(B_TURN + reach, lists_done), (B_TURN + reach + 1, find_blocks)]
    stages.sort(key=lambda pair: pair[0])
    for tick in range(2 * reach - 1):
        a_tick(tick)
        while stages and stages[0][0] <= tick:
            stages.pop(0)[1]()
    for _, stage in stages:
        stage()
    a_done()

    def pass_on(n, value, step):
        parts_out[n] = value.astype(jnp.bfloat16)
        return send(parts_out.at[n], parts_in.at[n], at_x(step))

    def taken(n, link):
        arrived(parts_in.at[n], link)
        return parts_in[n].astype(jnp.float32)

    up = pass_on(0, product(2, 0), 1)
    down = pass_on(1, product(2, 1), -1)
    below = pass_on(2, product(1, 1), 1)
    above = pass_on(3, product(3, 0), -1)
    kept[0] = product(1, 0)
    kept[1] = product(3, 1)
    out[0] = product(0, 0)
    out[1] = product(0, 1)
    up = pass_on(4, kept[0] + taken(0, up), 1)
    down = pass_on(5, kept[1] + taken(1, down), -1)
    out[1] += taken(2, below)
    out[0] += taken(3, above)
    for slot, (n, link) in enumerate(((4, up), (5, down))):
        s = high * 2 * x_count + 2 * x + slot
        out[slot] = jnp.where(s < c_cnt[0, 0], out[slot] + taken(n, link), 0.0)
    for copy in [*sent, *a_flying.values(), *lists_flying.values()]:
        copy.wait_send()
    mid = b_hop.at[0, mid_rows]
    pltpu.make_async_copy(mid, mid, send_sem.at[mid_send]).wait()

    @pl.when(relays)
    def _():
        for copy in mid_relays():
            copy.wait_send()


def on_device(a_values, a_index, a_count, b_values, b_index, b_count, c_index, c_count):
    row_count, col_count = lax.axis_size("row"), lax.axis_size("col")
    x_count = lax.axis_size("layer_1")
    assert row_count == 8 and x_count == 4
    z_count = 2 * col_count
    block = a_values.shape[-1]
    dtype = a_values.dtype
    far_memory = pl.BlockSpec(memory_space=pltpu.HBM)
    vmem = pl.BlockSpec(memory_space=pltpu.VMEM)
    lists = (
        a_index[0, 0, 0],
        a_count[0, 0][None],
        b_index[0, 0, 0],
        b_count[0, 0][None],
        c_index[0, 0],
        c_count,
    )
    result = pl.pallas_call(
        functools.partial(kernel, (row_count, col_count, x_count)),
        out_shape=jax.ShapeDtypeStruct((2, block, block), jnp.float32),
        in_specs=[far_memory] * 8,
        out_specs=vmem,
        scratch_shapes=[pltpu.SMEM(x.shape, jnp.int32) for x in lists]
        + [
            pltpu.VMEM((block, 2, block), dtype),
            pltpu.VMEM((2 * z_count, block, block), dtype),
            pltpu.VMEM((z_count, 1, 128), jnp.int32),
            pltpu.SMEM((z_count, 1, 128), jnp.int32),
            pltpu.VMEM((2 * row_count, block, block), dtype),
            pltpu.VMEM((row_count, 1, 128), jnp.int32),
            pltpu.SMEM((row_count, 1, 128), jnp.int32),
            pltpu.VMEM((3, block, block), dtype),
            pltpu.VMEM((row_count, block, block), dtype),
            pltpu.VMEM((2, block, block), jnp.float32),
            pltpu.VMEM((6, block, block), dtype),
            pltpu.VMEM((6, block, block), dtype),
            pltpu.SemaphoreType.DMA((10,)),
            pltpu.SemaphoreType.DMA((LINKS,)),
            pltpu.SemaphoreType.DMA((LINKS,)),
            pltpu.SemaphoreType.DMA((2 * RING,)),
            pltpu.SemaphoreType.DMA((2 * RING,)),
            pltpu.SemaphoreType.DMA((2 * LISTS,)),
            pltpu.SemaphoreType.DMA((2 * LISTS,)),
        ],
        compiler_params=pltpu.CompilerParams(
            collective_id=0, has_side_effects=True, vmem_limit_bytes=40 * 1024 * 1024
        ),
    )(
        *(pltpu.with_memory_space_constraint(v, pltpu.HBM) if v.size > 1 else v for v in lists),
        *(pltpu.with_memory_space_constraint(v[0, 0, 0], pltpu.HBM) for v in (a_values, b_values)),
    )
    return result[None, None]


def solution(mesh):
    highs = 2
    split = Mesh(
        mesh.devices.reshape(mesh.shape["row"], mesh.shape["col"], highs, mesh.shape["layer"] // highs),
        ("row", "col", "layer_0", "layer_1"),
    )
    return jax.shard_map(
        on_device,
        mesh=split,
        in_specs=(
            P("row", LAYER, "col", None, None, None),
            P("row", LAYER, "col", None, None),
            P("row", LAYER, "col"),
            P(LAYER, "row", "col", None, None, None),
            P(LAYER, "row", "col", None, None),
            P(LAYER, "row", "col"),
            P("row", "col", None, None),
            P("row", "col"),
        ),
        out_specs=P("row", "col", LAYER, None, None),
        check_vma=False,
    )
```
